8 devices in a mesh: data: 1 (over z), dap2: 2 (over y), dap: 4 (over x, core).
Axes of the slice: x: 2, y: 2, z: 1, core: 2. Of those that a mesh axis runs over, the one named last changes fastest.
Arguments:
- pair_rep: bfloat16 [640, 640, 128], P(('data', 'dap2', 'dap'))
- pair_mask: int32 [640, 640], P(('data', 'dap2', 'dap'))
- norm_in: bfloat16 [6, 2, 2, 128], replicated
- norm_out: bfloat16 [6, 2, 2, 128], replicated
- w_ab: bfloat16 [6, 2, 128, 512], replicated
- w_gate: bfloat16 [6, 2, 128, 128], replicated
- w_out: bfloat16 [6, 2, 128, 128], replicated
Outputs:
- output: bfloat16 [640, 640, 128], P(('data', 'dap2', 'dap'))
All inputs are finite; a program needn't handle non-finite values.
Results may differ from the reference program's by a relative error of at most 0.0141214.
Values are sent between devices in bfloat16 or wider.
A program may use at most 1 GiB of HBM per device.

```python
import jax
import jax.numpy as jnp
from jax import lax

N_RES = 640
C_PAIR = 128
C_HID = 128
N_LAYERS = 6
LN_EPS = 1e-5


def setup_inputs(seed: int = 0, part: int = 0) -> dict:
    base_key = jax.random.key(seed)
    part_key = jax.random.fold_in(base_key, part)
    pair_key, mask_key = jax.random.split(part_key)
    weight_keys = jax.random.split(jax.random.key(seed + 17), 5)
    pair_rep = jax.random.normal(pair_key, (N_RES, N_RES, C_PAIR), jnp.float32).astype(jnp.bfloat16)
    keep_res = (jax.random.randint(mask_key, (N_RES,), 0, 16) != 0).astype(jnp.int32)
    pair_mask = keep_res[:, None] * keep_res[None, :]
    norm_base = jnp.array([1.0, 0.0], jnp.float32)[:, None]
    norm_in = (norm_base + 0.3 * jax.random.normal(weight_keys[0], (N_LAYERS, 2, 2, C_PAIR), jnp.float32)).astype(jnp.bfloat16)
    norm_out = (norm_base + 0.3 * jax.random.normal(weight_keys[1], (N_LAYERS, 2, 2, C_HID), jnp.float32)).astype(jnp.bfloat16)
    w_ab = (jax.random.normal(weight_keys[2], (N_LAYERS, 2, C_PAIR, 4 * C_HID), jnp.float32) * C_PAIR ** -0.5).astype(jnp.bfloat16)
    w_gate = (jax.random.normal(weight_keys[3], (N_LAYERS, 2, C_PAIR, C_PAIR), jnp.float32) * C_PAIR ** -0.5).astype(jnp.bfloat16)
    w_out = (jax.random.normal(weight_keys[4], (N_LAYERS, 2, C_HID, C_PAIR), jnp.float32) * (0.5 * C_HID ** -0.5)).astype(jnp.bfloat16)
    return {"pair_rep": pair_rep, "pair_mask": pair_mask, "norm_in": norm_in, "norm_out": norm_out, "w_ab": w_ab, "w_gate": w_gate, "w_out": w_out}


def layer_norm(values, gain_vec, shift_vec, norm_axis):
    mean_val = jnp.mean(values, axis=norm_axis, keepdims=True)
    centered = values - mean_val
    var_val = jnp.mean(centered * centered, axis=norm_axis, keepdims=True)
    return centered * lax.rsqrt(var_val + LN_EPS) * gain_vec + shift_vec


def tri_update(pair_cur, mask_f, norm_in, norm_out, w_ab, w_gate, w_out, outgoing):
    gain_in = norm_in[0].astype(jnp.float32)
    shift_in = norm_in[1].astype(jnp.float32)
    gain_out = norm_out[0].astype(jnp.float32)
    shift_out = norm_out[1].astype(jnp.float32)

    def row_inputs(row_args):
        x_row = layer_norm(row_args[0].astype(jnp.float32), gain_in, shift_in, -1).astype(jnp.bfloat16)
        proj_row = jnp.dot(x_row, w_ab, preferred_element_type=jnp.float32).reshape(N_RES, 4, C_HID)
        a_row = (row_args[1] * jax.nn.sigmoid(proj_row[:, 1]) * proj_row[:, 0]).astype(jnp.bfloat16)
        b_row = (row_args[1] * jax.nn.sigmoid(proj_row[:, 3]) * proj_row[:, 2]).astype(jnp.bfloat16)
        return a_row, b_row

    def out_channel(ab_pair):
        return jnp.dot(ab_pair[0], ab_pair[1].T, preferred_element_type=jnp.float32).astype(jnp.bfloat16)

    def in_channel(ab_pair):
        return jnp.dot(ab_pair[0].T, ab_pair[1], preferred_element_type=jnp.float32).astype(jnp.bfloat16)

    def row_output(row_args):
        pair_f = row_args[0].astype(jnp.float32)
        x_row = layer_norm(pair_f, gain_in, shift_in, -1).astype(jnp.bfloat16)
        y_row = layer_norm(row_args[1].astype(jnp.float32), gain_out, shift_out, -1).astype(jnp.bfloat16)
        update_val = jnp.dot(y_row, w_out, preferred_element_type=jnp.float32)
        gate_val = jax.nn.sigmoid(jnp.dot(x_row, w_gate, preferred_element_type=jnp.float32))
        return (pair_f + gate_val * update_val).astype(jnp.bfloat16)

    a_val, b_val = lax.map(row_inputs, (pair_cur, mask_f))
    channel_fn = out_channel if outgoing else in_channel
    tri_out = lax.map(channel_fn, (jnp.transpose(a_val, (2, 0, 1)), jnp.transpose(b_val, (2, 0, 1))))
    return lax.map(row_output, (pair_cur, jnp.transpose(tri_out, (1, 2, 0))))


def reference(pair_rep, pair_mask, norm_in, norm_out, w_ab, w_gate, w_out):
    mask_f = pair_mask.astype(jnp.float32)[:, :, None]

    def layer_step(pair_cur, params):
        pair_cur = tri_update(pair_cur, mask_f, params[0][0], params[1][0], params[2][0], params[3][0], params[4][0], True)
        pair_cur = tri_update(pair_cur, mask_f, params[0][1], params[1][1], params[2][1], params[3][1], params[4][1], False)
        return pair_cur, None

    return lax.scan(layer_step, pair_rep, (norm_in, norm_out, w_ab, w_gate, w_out))[0]
```

```python
import functools

import jax
import jax.numpy as jnp
from jax import lax
from jax.experimental import pallas as pl
from jax.experimental.pallas import tpu as pltpu
from jax.sharding import PartitionSpec as P

LN_EPS = 1e-5
ALL_ROWS = ("data", "dap2", "dap")
MESH = pl.DeviceIdType.MESH
NDEV = 8
CH = 128
SUB = CH // NDEV
RB = 16
LANES = 128
GSZ = 2
AHEAD = 3
VMEM_LIMIT = 62 * 1024 * 1024


def norm_cols(vals, gain, shift):
    mean_val = jnp.mean(vals, axis=0, keepdims=True)
    centered = vals - mean_val
    var_val = jnp.mean(centered * centered, axis=0, keepdims=True)
    return centered * lax.rsqrt(var_val + LN_EPS) * gain + shift


def sigmoid(vals):
    return 0.5 * jnp.tanh(0.5 * vals) + 0.5


def rows_kernel(do_c, do_a, ncol, *refs):
    refs = list(refs)
    z_ref = refs.pop(0)
    if do_c:
        t_ref, gip_ref, sip_ref, go_ref, so_ref, wg_ref, wo_ref = refs[:7]
        refs = refs[7:]
    if do_a:
        m_ref, gi_ref, si_ref, wab_ref = refs[:4]
        refs = refs[4:]
    if do_c:
        zo_ref = refs.pop(0)
    if do_a:
        ab_ref = refs.pop(0)
    x_ref, o_ref, g_ref = refs[:3]
    refs = refs[3:]
    if do_c:
        ts_ref, y_ref = refs[:2]
        refs = refs[2:]
    if do_a:
        p_ref, as_ref, bs_ref = refs

    if do_c:
        for c0 in range(0, CH, 16):
            for q in range(ncol // LANES):
                ts_ref[q, pl.ds(c0 * RB, 16 * RB), :] = t_ref[pl.ds(c0, 16), :, pl.ds(q * LANES, LANES)].astype(jnp.float32).reshape(16 * RB, LANES)

    def one_row(i, carry):
        chunks = [pl.ds(l0, LANES) for l0 in range(0, ncol, LANES)]
        if do_c:
            for q, ln in enumerate(chunks):
                x_ref[:, ln] = norm_cols(z_ref[i, :, ln].astype(jnp.float32), gip_ref[...], sip_ref[...]).astype(jnp.bfloat16)
                y_ref[:, ln] = norm_cols(ts_ref[q, pl.ds(i, CH, stride=RB), :], go_ref[...], so_ref[...]).astype(jnp.bfloat16)
            g_ref[...] = jnp.dot(wg_ref[...], x_ref[...], preferred_element_type=jnp.float32)
            o_ref[...] = jnp.dot(wo_ref[...], y_ref[...], preferred_element_type=jnp.float32)
            for q, ln in enumerate(chunks):
                new_z = z_ref[i, :, ln].astype(jnp.float32) + sigmoid(g_ref[:, ln]) * o_ref[:, ln]
                zo_ref[i, :, ln] = new_z.astype(jnp.bfloat16)
        src_ref = zo_ref if do_c else z_ref
        if do_a:
            for q, ln in enumerate(chunks):
                x_ref[:, ln] = norm_cols(src_ref[i, :, ln].astype(jnp.float32), gi_ref[...], si_ref[...]).astype(jnp.bfloat16)
            p_ref[...] = jnp.dot(wab_ref[...], x_ref[...], preferred_element_type=jnp.float32)
            for q, ln in enumerate(chunks):
                keep = m_ref[i, :, ln]
                as_ref[q, pl.ds(i, CH, stride=RB), :] = keep * sigmoid(p_ref[pl.ds(CH, CH), ln]) * p_ref[pl.ds(0, CH), ln]
                bs_ref[q, pl.ds(i, CH, stride=RB), :] = keep * sigmoid(p_ref[pl.ds(3 * CH, CH), ln]) * p_ref[pl.ds(2 * CH, CH), ln]
        return carry

    lax.fori_loop(0, RB, one_row, 0)
    if do_a:
        for d in range(NDEV):
            for s_ref, u in ((as_ref, 0), (bs_ref, 1)):
                for q in range(ncol // LANES):
                    ab_ref[d, :, u, :, pl.ds(q * LANES, LANES)] = s_ref[q, pl.ds(d * SUB * RB, SUB * RB), :].reshape(SUB, RB, LANES).astype(jnp.bfloat16)


def rows_call(do_c, do_a, z, t, mask, cw, aw):
    nrow, _, ncol = z.shape
    row_blk = pl.BlockSpec((RB, CH, ncol), lambda r: (r, 0, 0))

    def whole(arr):
        return pl.BlockSpec(arr.shape, lambda r: (0,) * arr.ndim)

    args, in_specs, outs, out_specs = [z], [row_blk], [], []
    scratch = [pltpu.VMEM((CH, ncol), jnp.bfloat16), pltpu.VMEM((CH, ncol), jnp.float32), pltpu.VMEM((CH, ncol), jnp.float32)]
    if do_c:
        args += [t.reshape(CH, nrow, ncol), *cw]
        in_specs += [pl.BlockSpec((CH, RB, ncol), lambda r: (0, r, 0))] + [whole(w) for w in cw]
        outs.append(jax.ShapeDtypeStruct(z.shape, jnp.bfloat16))
        out_specs.append(row_blk)
        scratch += [pltpu.VMEM((ncol // LANES, CH * RB, LANES), jnp.float32), pltpu.VMEM((CH, ncol), jnp.bfloat16)]
    if do_a:
        args += [mask, *aw]
        in_specs += [pl.BlockSpec((RB, 1, ncol), lambda r: (r, 0, 0))] + [whole(w) for w in aw]
        outs.append(jax.ShapeDtypeStruct((NDEV, SUB, 2, nrow, ncol), jnp.bfloat16))
        out_specs.append(pl.BlockSpec((NDEV, SUB, 2, RB, ncol), lambda r: (0, 0, 0, r, 0)))
        scratch += [pltpu.VMEM((4 * CH, ncol), jnp.float32), pltpu.VMEM((ncol // LANES, CH * RB, LANES), jnp.float32), pltpu.VMEM((ncol // LANES, CH * RB, LANES), jnp.float32)]
    return pl.pallas_call(
        functools.partial(rows_kernel, do_c, do_a, ncol),
        grid=(nrow // RB,),
        in_specs=in_specs,
        out_specs=out_specs,
        out_shape=outs,
        scratch_shapes=scratch,
        compiler_params=pltpu.CompilerParams(dimension_semantics=("arbitrary",), vmem_limit_bytes=VMEM_LIMIT),
        name="rows",
    )(*args)


def tri_kernel(outgoing, nrow, ncol, ab_ref, t_ref, recv, tbuf, s_ab, r_ab, s_t, r_t, l_ab, l_t):
    y_id = lax.axis_index("dap2")
    xc_id = lax.axis_index("dap")
    z_id = lax.axis_index("data")
    x_id, c_id = xc_id // 2, xc_id % 2
    me = y_id * 4 + xc_id
    ngroup = SUB // GSZ

    def peer(d):
        py, px, pc = (y_id + d // 4) % 2, (x_id + (d // 2) % 2) % 2, (c_id + d % 2) % 2
        return (z_id, py, px * 2 + pc), py * 4 + px * 2 + pc

    def chans(g):
        return pl.ds(g * GSZ, GSZ)

    def ab_copy(g, d):
        dev, num = peer(d)
        return pltpu.make_async_remote_copy(
            src_ref=ab_ref.at[num, chans(g)], dst_ref=recv.at[me, chans(g)],
            send_sem=s_ab.at[g, d], recv_sem=r_ab.at[g, d], device_id=dev, device_id_type=MESH)

    def t_copy(g, d):
        dev, num = peer(d)
        return pltpu.make_async_remote_copy(
            src_ref=tbuf.at[num, chans(g)], dst_ref=t_ref.at[me, chans(g)],
            send_sem=s_t.at[g, d], recv_sem=r_t.at[g, d], device_id=dev, device_id_type=MESH)

    def own_ab(g):
        return pltpu.make_async_copy(ab_ref.at[me, chans(g)], recv.at[me, chans(g)], l_ab.at[g])

    def own_t(g):
        return pltpu.make_async_copy(tbuf.at[me, chans(g)], t_ref.at[me, chans(g)], l_t.at[g])

    order = (6, 4, 2, 7, 5, 3, 1)

    barrier = pltpu.get_barrier_semaphore()
    for d in range(1, NDEV):
        pl.semaphore_signal(barrier, inc=1, device_id=peer(d)[0], device_id_type=MESH)
    pl.semaphore_wait(barrier, NDEV - 1)

    def send_group(g):
        for d in order:
            ab_copy(g, d).start()
        own_ab(g).start()

    for g in range(AHEAD):
        send_group(g)

    def group_step(g, carry):
        @pl.when(g < ngroup - AHEAD)
        def _():
            send_group(g + AHEAD)

        for d in order:
            ab_copy(g, d).wait_recv()
        own_ab(g).wait()
        for q in range(GSZ):
            ch = g * GSZ + q
            a_val = recv[:, ch, 0].reshape(NDEV * nrow, ncol)
            b_val = recv[:, ch, 1].reshape(NDEV * nrow, ncol)
            dims = (((1,), (1,)), ((), ())) if outgoing else (((0,), (0,)), ((), ()))
            t_val = lax.dot_general(a_val, b_val, dims, preferred_element_type=jnp.float32)
            tbuf[:, ch] = t_val.astype(jnp.bfloat16).reshape(NDEV, nrow, ncol)
        for d in order:
            t_copy(g, d).start()
        own_t(g).start()
        return carry

    lax.fori_loop(0, ngroup, group_step, 0)

    def drain(g, carry):
        for d in order:
            t_copy(g, d).wait_recv()
            t_copy(g, d).wait_send()
            ab_copy(g, d).wait_send()
        own_t(g).wait()
        return carry

    lax.fori_loop(0, ngroup, drain, 0)


def tri_call(outgoing, ab):
    _, _, _, nrow, ncol = ab.shape
    ngroup = SUB // GSZ
    sems = pltpu.SemaphoreType.DMA((ngroup, NDEV))
    return pl.pallas_call(
        functools.partial(tri_kernel, outgoing, nrow, ncol),
        in_specs=[pl.BlockSpec(memory_space=pl.ANY)],
        out_specs=pl.BlockSpec(memory_space=pl.ANY),
        out_shape=jax.ShapeDtypeStruct((NDEV, SUB, nrow, ncol), jnp.bfloat16),
        scratch_shapes=[
            pltpu.VMEM((NDEV, SUB, 2, nrow, ncol), jnp.bfloat16),
            pltpu.VMEM((NDEV, SUB, nrow, ncol), jnp.bfloat16),
            sems, sems, sems, sems,
            pltpu.SemaphoreType.DMA((ngroup,)), pltpu.SemaphoreType.DMA((ngroup,)),
        ],
        compiler_params=pltpu.CompilerParams(collective_id=0 if outgoing else 1, has_side_effects=True, vmem_limit_bytes=VMEM_LIMIT),
        name="tri_out" if outgoing else "tri_in",
    )(ab)


def solution(mesh):
    row_spec = P(ALL_ROWS, None, None)
    mask_spec = P(ALL_ROWS, None)

    def local_stack(pair_rep, pair_mask, norm_in, norm_out, w_ab, w_gate, w_out):
        mask_f = pair_mask.astype(jnp.float32)[:, None, :]
        norm_in = norm_in.astype(jnp.float32)[..., None]
        norm_out = norm_out.astype(jnp.float32)[..., None]
        w_ab = jnp.swapaxes(w_ab, -1, -2)
        w_gate = jnp.swapaxes(w_gate, -1, -2)
        w_out = jnp.swapaxes(w_out, -1, -2)
        n_layers = w_ab.shape[0]

        def cw(l, u):
            return (norm_in[l, u, 0], norm_in[l, u, 1], norm_out[l, u, 0], norm_out[l, u, 1], w_gate[l, u], w_out[l, u])

        def aw(l, u):
            return (norm_in[l, u, 0], norm_in[l, u, 1], w_ab[l, u])

        def layer(l, z, ab):
            t = tri_call(True, ab)
            z, ab = rows_call(True, True, z, t, mask_f, cw(l, 0), aw(l, 1))
            return z, tri_call(False, ab)

        def body(l, state):
            z, t = layer(l, *state)
            return tuple(rows_call(True, True, z, t, mask_f, cw(l, 1), aw(l + 1, 0)))

        z = jnp.swapaxes(pair_rep, 1, 2)
        ab, = rows_call(False, True, z, None, mask_f, None, aw(0, 0))
        z, ab = lax.fori_loop(0, n_layers - 1, body, (z, ab))
        z, t = layer(n_layers - 1, z, ab)
        z, = rows_call(True, False, z, t, mask_f, cw(n_layers - 1, 1), None)
        return jnp.swapaxes(z, 1, 2)

    return jax.shard_map(local_stack, mesh=mesh, in_specs=(row_spec, mask_spec, P(), P(), P(), P(), P()), out_specs=row_spec, check_vma=False)
```

```python
import functools

import jax
import jax.numpy as jnp
from jax import lax
from jax.experimental import pallas as pl
from jax.experimental.pallas import tpu as pltpu
from jax.sharding import PartitionSpec as P

LN_EPS = 1e-5
ALL_ROWS = ("data", "dap2", "dap")
MESH = pl.DeviceIdType.MESH
NDEV = 8
CH = 128
SUB = CH // NDEV
RB = 16
LANES = 128
VMEM_LIMIT = 62 * 1024 * 1024
ORDER = (6, 4, 2, 7, 5, 3, 1)


def norm_cols(vals, gain, shift):
    mean_val = jnp.mean(vals, axis=0, keepdims=True)
    centered = vals - mean_val
    var_val = jnp.mean(centered * centered, axis=0, keepdims=True)
    return centered * lax.rsqrt(var_val + LN_EPS) * gain + shift


def sigmoid(vals):
    return 0.5 * jnp.tanh(0.5 * vals) + 0.5


def update_kernel(do_c, do_a, outgoing, nrow, ncol, *refs):
    refs = list(refs)

    def take(count):
        out = refs[:count]
        del refs[:count]
        return out

    z_ref, = take(1)
    if do_c:
        t_ref, gip_ref, sip_ref, go_ref, so_ref, wg_ref, wo_ref = take(7)
    if do_a:
        m_ref, gi_ref, si_ref, wab_ref = take(4)
    if do_c:
        zo_ref, tr_ref = take(2)
    if do_a:
        tn_ref, ab_ref = take(2)
    zbuf, scr, x_ref, l_z = take(4)
    if do_c:
        o_ref, g_ref, y_ref, tblk, s_t, r_t, l_t = take(7)
    if do_a:
        p_ref, scr_b, abblk, recv, tst, s_ab, r_ab, l_ab, l_st, l_tn = take(10)

    y_id = lax.axis_index("dap2")
    xc_id = lax.axis_index("dap")
    z_id = lax.axis_index("data")
    x_id, c_id = xc_id // 2, xc_id % 2
    me = y_id * 4 + xc_id
    nblk = nrow // RB
    nlane = ncol // LANES

    def peer(d):
        py, px, pc = (y_id + d // 4) % 2, (x_id + (d // 2) % 2) % 2, (c_id + d % 2) % 2
        return (z_id, py, px * 2 + pc), py * 4 + px * 2 + pc

    def rows(r):
        return pl.ds(r * RB, RB)

    def t_copy(r, d):
        dev, num = peer(d)
        return pltpu.make_async_remote_copy(
            src_ref=t_ref.at[num, :, rows(r)], dst_ref=tr_ref.at[me, :, rows(r)],
            send_sem=s_t.at[r, d], recv_sem=r_t.at[r, d], device_id=dev, device_id_type=MESH)

    def ab_copy(r, d):
        dev, num = peer(d)
        return pltpu.make_async_remote_copy(
            src_ref=ab_ref.at[num, :, :, rows(r)], dst_ref=recv.at[me, :, :, rows(r)],
            send_sem=s_ab.at[r, d], recv_sem=r_ab.at[r, d], device_id=dev, device_id_type=MESH)

    def own_ab(r):
        return pltpu.make_async_copy(ab_ref.at[me, :, :, rows(r)], recv.at[me, :, :, rows(r)], l_ab.at[r])

    def stage_ab(r):
        return pltpu.make_async_copy(abblk, ab_ref.at[:, :, :, rows(r)], l_st)

    def load_t(r, d):
        num = peer(d)[1]
        src_ref = t_ref if d == 0 else tr_ref
        return pltpu.make_async_copy(src_ref.at[num, :, rows(r)], tblk.at[num], l_t.at[d])

    def load_z(r):
        return pltpu.make_async_copy(z_ref.at[rows(r)], zbuf, l_z)

    def store_z(r):
        return pltpu.make_async_copy(zbuf, zo_ref.at[rows(r)], l_z)

    barrier = pltpu.get_barrier_semaphore()
    for d in range(1, NDEV):
        pl.semaphore_signal(barrier, inc=1, device_id=peer(d)[0], device_id_type=MESH)
    pl.semaphore_wait(barrier, NDEV - 1)

    if do_c:
        for r in range(nblk):
            for d in ORDER:
                t_copy(r, d).start()

    chunks = [pl.ds(l0, LANES) for l0 in range(0, ncol, LANES)]

    def one_row(r, i):
        if do_c:
            for q, ln in enumerate(chunks):
                x_ref[:, ln] = norm_cols(zbuf[i, :, ln].astype(jnp.float32), gip_ref[...], sip_ref[...]).astype(jnp.bfloat16)
                y_ref[:, ln] = norm_cols(scr[q, pl.ds(i, CH, stride=RB), :], go_ref[...], so_ref[...]).astype(jnp.bfloat16)
            g_ref[...] = jnp.dot(wg_ref[...], x_ref[...], preferred_element_type=jnp.float32)
            o_ref[...] = jnp.dot(wo_ref[...], y_ref[...], preferred_element_type=jnp.float32)
            for q, ln in enumerate(chunks):
                new_z = zbuf[i, :, ln].astype(jnp.float32) + sigmoid(g_ref[:, ln]) * o_ref[:, ln]
                zbuf[i, :, ln] = new_z.astype(jnp.bfloat16)
        if do_a:
            for q, ln in enumerate(chunks):
                x_ref[:, ln] = norm_cols(zbuf[i, :, ln].astype(jnp.float32), gi_ref[...], si_ref[...]).astype(jnp.bfloat16)
            p_ref[...] = jnp.dot(wab_ref[...], x_ref[...], preferred_element_type=jnp.float32)
            for q, ln in enumerate(chunks):
                keep = m_ref[r * RB + i, :, ln]
                scr[q, pl.ds(i, CH, stride=RB), :] = keep * sigmoid(p_ref[pl.ds(CH, CH), ln]) * p_ref[pl.ds(0, CH), ln]
                scr_b[q, pl.ds(i, CH, stride=RB), :] = keep * sigmoid(p_ref[pl.ds(3 * CH, CH), ln]) * p_ref[pl.ds(2 * CH, CH), ln]

    def block_step(r, carry):
        load_z(r).start()
        if do_c:
            for d in ORDER:
                t_copy(r, d).wait_recv()
            for d in range(NDEV):
                load_t(r, d).start()
            for d in range(NDEV):
                load_t(r, d).wait()
            for s in range(NDEV):
                for q, ln in enumerate(chunks):
                    scr[q, pl.ds(s * SUB * RB, SUB * RB), :] = tblk[s, :, :, ln].astype(jnp.float32).reshape(SUB * RB, LANES)
        load_z(r).wait()

        def row_step(i, inner):
            one_row(r, i)
            return inner

        lax.fori_loop(0, RB, row_step, 0)
        if do_c:
            store_z(r).start()
        if do_a:
            for d in range(NDEV):
                for s_ref, u in ((scr, 0), (scr_b, 1)):
                    for q, ln in enumerate(chunks):
                        abblk[d, :, u, :, ln] = s_ref[q, pl.ds(d * SUB * RB, SUB * RB), :].reshape(SUB, RB, LANES).astype(jnp.bfloat16)
            stage_ab(r).start()
            stage_ab(r).wait()
            for d in ORDER:
                ab_copy(r, d).start()
            own_ab(r).start()
        if do_c:
            store_z(r).wait()
        return carry

    lax.fori_loop(0, nblk, block_step, 0)

    if do_a:
        def wait_ab(r, carry):
            for d in ORDER:
                ab_copy(r, d).wait_recv()
            own_ab(r).wait()
            return carry

        lax.fori_loop(0, nblk, wait_ab, 0)

        def put_t(ch):
            return pltpu.make_async_copy(tst.at[ch % 2], tn_ref.at[:, ch], l_tn.at[ch % 2])

        def chan_step(ch, carry):
            a_val = recv[:, ch, 0].reshape(NDEV * nrow, ncol)
            b_val = recv[:, ch, 1].reshape(NDEV * nrow, ncol)
            dims = (((1,), (1,)), ((), ())) if outgoing else (((0,), (0,)), ((), ()))
            t_val = lax.dot_general(a_val, b_val, dims, preferred_element_type=jnp.float32)

            @pl.when(ch >= 2)
            def _():
                put_t(ch - 2).wait()

            tst[ch % 2] = t_val.astype(jnp.bfloat16).reshape(NDEV, nrow, ncol)
            put_t(ch).start()
            return carry

        lax.fori_loop(0, SUB, chan_step, 0)
        put_t(SUB - 2).wait()
        put_t(SUB - 1).wait()

    def drain(r, carry):
        for d in ORDER:
            if do_c:
                t_copy(r, d).wait_send()
            if do_a:
                ab_copy(r, d).wait_send()
        return carry

    lax.fori_loop(0, nblk, drain, 0)


def update_call(do_c, do_a, outgoing, cid, z, t, mask, cw, aw):
    nrow, _, ncol = z.shape
    nblk = nrow // RB
    hbm = pl.BlockSpec(memory_space=pl.ANY)
    vmem = pl.BlockSpec(memory_space=pltpu.VMEM)
    sems = pltpu.SemaphoreType.DMA((nblk, NDEV))
    strided = pltpu.VMEM((ncol // LANES, CH * RB, LANES), jnp.float32)
    t_shape = jax.ShapeDtypeStruct((NDEV, SUB, nrow, ncol), jnp.bfloat16)
    args, in_specs, outs = [z], [hbm], []
    scratch = [pltpu.VMEM((RB, CH, ncol), jnp.bfloat16), strided, pltpu.VMEM((CH, ncol), jnp.bfloat16), pltpu.SemaphoreType.DMA]
    if do_c:
        args += [t, *cw]
        in_specs += [hbm] + [vmem] * len(cw)
        outs += [jax.ShapeDtypeStruct(z.shape, jnp.bfloat16), t_shape]
        scratch += [pltpu.VMEM((CH, ncol), jnp.float32), pltpu.VMEM((CH, ncol), jnp.float32), pltpu.VMEM((CH, ncol), jnp.bfloat16),
                    pltpu.VMEM((NDEV, SUB, RB, ncol), jnp.bfloat16), sems, sems, pltpu.SemaphoreType.DMA((NDEV,))]
    if do_a:
        args += [mask, *aw]
        in_specs += [vmem] * (1 + len(aw))
        outs += [t_shape, jax.ShapeDtypeStruct((NDEV, SUB, 2, nrow, ncol), jnp.bfloat16)]
        scratch += [pltpu.VMEM((4 * CH, ncol), jnp.float32), strided, pltpu.VMEM((NDEV, SUB, 2, RB, ncol), jnp.bfloat16),
                    pltpu.VMEM((NDEV, SUB, 2, nrow, ncol), jnp.bfloat16), pltpu.VMEM((2, NDEV, nrow, ncol), jnp.bfloat16),
                    sems, sems, pltpu.SemaphoreType.DMA((nblk,)), pltpu.SemaphoreType.DMA, pltpu.SemaphoreType.DMA((2,))]
    return pl.pallas_call(
        functools.partial(update_kernel, do_c, do_a, outgoing, nrow, ncol),
        in_specs=in_specs,
        out_specs=[hbm] * len(outs),
        out_shape=outs,
        scratch_shapes=scratch,
        compiler_params=pltpu.CompilerParams(collective_id=cid, has_side_effects=True, vmem_limit_bytes=VMEM_LIMIT),
        name="update",
    )(*args)


def solution(mesh):
    row_spec = P(ALL_ROWS, None, None)
    mask_spec = P(ALL_ROWS, None)

    def local_stack(pair_rep, pair_mask, norm_in, norm_out, w_ab, w_gate, w_out):
        mask_f = pair_mask.astype(jnp.float32)[:, None, :]
        norm_in = norm_in.astype(jnp.float32)[..., None]
        norm_out = norm_out.astype(jnp.float32)[..., None]
        w_ab = jnp.swapaxes(w_ab, -1, -2)
        w_gate = jnp.swapaxes(w_gate, -1, -2)
        w_out = jnp.swapaxes(w_out, -1, -2)
        n_layers = w_ab.shape[0]

        def cw(l, u):
            return (norm_in[l, u, 0], norm_in[l, u, 1], norm_out[l, u, 0], norm_out[l, u, 1], w_gate[l, u], w_out[l, u])

        def aw(l, u):
            return (norm_in[l, u, 0], norm_in[l, u, 1], w_ab[l, u])

        def to_incoming(l, z, t):
            z, _, t, _ = update_call(True, True, False, 1, z, t, mask_f, cw(l, 0), aw(l, 1))
            return z, t

        def body(l, state):
            z, t = to_incoming(l, *state)
            z, _, t, _ = update_call(True, True, True, 2, z, t, mask_f, cw(l, 1), aw(l + 1, 0))
            return z, t

        z = jnp.swapaxes(pair_rep, 1, 2)
        t, _ = update_call(False, True, True, 0, z, None, mask_f, None, aw(0, 0))
        z, t = lax.fori_loop(0, n_layers - 1, body, (z, t))
        z, t = to_incoming(n_layers - 1, z, t)
        z, _ = update_call(True, False, False, 3, z, t, mask_f, cw(n_layers - 1, 1), None)
        return jnp.swapaxes(z, 1, 2)

    return jax.shard_map(local_stack, mesh=mesh, in_specs=(row_spec, mask_spec, P(), P(), P(), P(), P()), out_specs=row_spec, check_vma=False)
```

```python
import functools

import jax
import jax.numpy as jnp
from jax import lax
from jax.experimental import pallas as pl
from jax.experimental.pallas import tpu as pltpu
from jax.sharding import PartitionSpec as P

LN_EPS = 1e-5
ALL_ROWS = ("data", "dap2", "dap")
MESH = pl.DeviceIdType.MESH
NDEV = 8
CH = 128
SUB = CH // NDEV
RB = 16
LANES = 128
VMEM_LIMIT = 62 * 1024 * 1024
ORDER = (6, 4, 2, 7, 5, 3, 1)


def norm_cols(vals, gain, shift):
    mean_val = jnp.mean(vals, axis=0, keepdims=True)
    centered = vals - mean_val
    var_val = jnp.mean(centered * centered, axis=0, keepdims=True)
    return centered * lax.rsqrt(var_val + LN_EPS) * gain + shift


def sigmoid(vals):
    return 0.5 * jnp.tanh(0.5 * vals) + 0.5


def first_and_rest(do_c):
    return (4, ((4, 4), (8, 4), (12, 2), (14, 2))) if do_c else (8, ((8, 4), (12, 2), (14, 2)))


def update_kernel(do_c, do_a, outgoing, nrow, ncol, *refs):
    refs = list(refs)

    def take(count):
        out = refs[:count]
        del refs[:count]
        return out

    z_ref, = take(1)
    if do_c:
        t_ref, = take(1)
    if do_a:
        m_ref, = take(1)
    v_ref, w_ref = take(2)
    if do_c:
        zo_ref, tr_ref = take(2)
    if do_a:
        tn_ref, ab_ref = take(2)
    zbuf, scr, x_ref, l_z = take(4)
    if do_c:
        o_ref, g_ref, y_ref, tblk, s_t, r_t, l_t = take(7)
    if do_a:
        p_ref, scr_b, abblk, recv, tst, s_ab, r_ab, l_ab, l_st, l_tn, s_rest, r_rest, l_rest = take(13)

    y_id = lax.axis_index("dap2")
    xc_id = lax.axis_index("dap")
    z_id = lax.axis_index("data")
    x_id, c_id = xc_id // 2, xc_id % 2
    me = y_id * 4 + xc_id
    nblk = nrow // RB
    first, rest = first_and_rest(do_c)

    def peer(d):
        py, px, pc = (y_id + d // 4) % 2, (x_id + (d // 2) % 2) % 2, (c_id + d % 2) % 2
        return (z_id, py, px * 2 + pc), py * 4 + px * 2 + pc

    def rows(r):
        return pl.ds(r * RB, RB)

    def t_copy(r, d):
        dev, num = peer(d)
        return pltpu.make_async_remote_copy(
            src_ref=t_ref.at[num, :, rows(r)], dst_ref=tr_ref.at[me, :, rows(r)],
            send_sem=s_t.at[r, d], recv_sem=r_t.at[r, d], device_id=dev, device_id_type=MESH)

    def ab_copy(r, d):
        dev, num = peer(d)
        return pltpu.make_async_remote_copy(
            src_ref=ab_ref.at[num, pl.ds(0, first), :, rows(r)], dst_ref=recv.at[me, pl.ds(0, first), :, rows(r)],
            send_sem=s_ab.at[r, d], recv_sem=r_ab.at[r, d], device_id=dev, device_id_type=MESH)

    def own_ab(r):
        return pltpu.make_async_copy(ab_ref.at[me, pl.ds(0, first), :, rows(r)], recv.at[me, pl.ds(0, first), :, rows(r)], l_ab.at[r])

    def rest_copy(g, d):
        dev, num = peer(d)
        return pltpu.make_async_remote_copy(
            src_ref=ab_ref.at[num, pl.ds(*rest[g])], dst_ref=recv.at[me, pl.ds(*rest[g])],
            send_sem=s_rest.at[g, d], recv_sem=r_rest.at[g, d], device_id=dev, device_id_type=MESH)

    def own_rest():
        return pltpu.make_async_copy(ab_ref.at[me, pl.ds(first, SUB - first)], recv.at[me, pl.ds(first, SUB - first)], l_rest)

    def stage_ab(r):
        return pltpu.make_async_copy(abblk, ab_ref.at[:, :, :, rows(r)], l_st)

    def load_t(r, d):
        num = peer(d)[1]
        src_ref = t_ref if d == 0 else tr_ref
        return pltpu.make_async_copy(src_ref.at[num, :, rows(r)], tblk.at[num], l_t.at[d])

    def load_z(r):
        return pltpu.make_async_copy(z_ref.at[rows(r)], zbuf, l_z)

    def store_z(r):
        return pltpu.make_async_copy(zbuf, zo_ref.at[rows(r)], l_z)

    barrier = pltpu.get_barrier_semaphore()
    for d in range(1, NDEV):
        pl.semaphore_signal(barrier, inc=1, device_id=peer(d)[0], device_id_type=MESH)
    pl.semaphore_wait(barrier, NDEV - 1)

    if do_c:
        for r in range(nblk):
            for d in ORDER:
                t_copy(r, d).start()

    chunks = [pl.ds(l0, LANES) for l0 in range(0, ncol, LANES)]

    def one_row(r, i):
        if do_c:
            for q, ln in enumerate(chunks):
                x_ref[:, ln] = norm_cols(zbuf[i, :, ln].astype(jnp.float32), v_ref[:, 0:1], v_ref[:, 1:2]).astype(jnp.bfloat16)
                y_ref[:, ln] = norm_cols(scr[q, pl.ds(i, CH, stride=RB), :], v_ref[:, 2:3], v_ref[:, 3:4]).astype(jnp.bfloat16)
            g_ref[...] = jnp.dot(w_ref[pl.ds(0, CH), :], x_ref[...], preferred_element_type=jnp.float32)
            o_ref[...] = jnp.dot(w_ref[pl.ds(CH, CH), :], y_ref[...], preferred_element_type=jnp.float32)
            for q, ln in enumerate(chunks):
                new_z = zbuf[i, :, ln].astype(jnp.float32) + sigmoid(g_ref[:, ln]) * o_ref[:, ln]
                zbuf[i, :, ln] = new_z.astype(jnp.bfloat16)
        if do_a:
            for q, ln in enumerate(chunks):
                x_ref[:, ln] = norm_cols(zbuf[i, :, ln].astype(jnp.float32), v_ref[:, 4:5], v_ref[:, 5:6]).astype(jnp.bfloat16)
            p_ref[...] = jnp.dot(w_ref[pl.ds(2 * CH, 4 * CH), :], x_ref[...], preferred_element_type=jnp.float32)
            for q, ln in enumerate(chunks):
                keep = m_ref[r * RB + i, :, ln]
                scr[q, pl.ds(i, CH, stride=RB), :] = keep * sigmoid(p_ref[pl.ds(CH, CH), ln]) * p_ref[pl.ds(0, CH), ln]
                scr_b[q, pl.ds(i, CH, stride=RB), :] = keep * sigmoid(p_ref[pl.ds(3 * CH, CH), ln]) * p_ref[pl.ds(2 * CH, CH), ln]

    def block_step(r, carry):
        load_z(r).start()
        if do_c:
            for d in ORDER:
                t_copy(r, d).wait_recv()
            for d in range(NDEV):
                load_t(r, d).start()
            for d in range(NDEV):
                load_t(r, d).wait()
            for s in range(NDEV):
                for q, ln in enumerate(chunks):
                    scr[q, pl.ds(s * SUB * RB, SUB * RB), :] = tblk[s, :, :, ln].astype(jnp.float32).reshape(SUB * RB, LANES)
        load_z(r).wait()

        def row_step(i, inner):
            one_row(r, i)
            return inner

        lax.fori_loop(0, RB, row_step, 0)
        if do_c:
            store_z(r).start()
        if do_a:
            for d in range(NDEV):
                for s_ref, u in ((scr, 0), (scr_b, 1)):
                    for q, ln in enumerate(chunks):
                        abblk[d, :, u, :, ln] = s_ref[q, pl.ds(d * SUB * RB, SUB * RB), :].reshape(SUB, RB, LANES).astype(jnp.bfloat16)
            stage_ab(r).start()
            stage_ab(r).wait()
            for d in ORDER:
                ab_copy(r, d).start()
            own_ab(r).start()
        if do_c:
            store_z(r).wait()
        return carry

    lax.fori_loop(0, nblk, block_step, 0)

    if do_a:
        for g in range(len(rest)):
            for d in ORDER:
                rest_copy(g, d).start()
        own_rest().start()

        def wait_ab(r, carry):
            for d in ORDER:
                ab_copy(r, d).wait_recv()
            own_ab(r).wait()
            return carry

        lax.fori_loop(0, nblk, wait_ab, 0)
        own_rest().wait()

        def put_t(ch):
            return pltpu.make_async_copy(tst.at[ch % 2], tn_ref.at[:, ch], l_tn.at[ch % 2])

        def chan_step(ch, carry):
            for g in range(len(rest)):
                @pl.when(ch == rest[g][0])
                def _(g=g):
                    for d in ORDER:
                        rest_copy(g, d).wait_recv()

            a_val = recv[:, ch, 0].reshape(NDEV * nrow, ncol)
            b_val = recv[:, ch, 1].reshape(NDEV * nrow, ncol)
            dims = (((1,), (1,)), ((), ())) if outgoing else (((0,), (0,)), ((), ()))
            t_val = lax.dot_general(a_val, b_val, dims, preferred_element_type=jnp.float32)

            @pl.when(ch >= 2)
            def _():
                put_t(ch - 2).wait()

            tst[ch % 2] = t_val.astype(jnp.bfloat16).reshape(NDEV, nrow, ncol)
            put_t(ch).start()
            return carry

        lax.fori_loop(0, SUB, chan_step, 0)
        put_t(SUB - 2).wait()
        put_t(SUB - 1).wait()

    def drain(r, carry):
        for d in ORDER:
            if do_c:
                t_copy(r, d).wait_send()
            if do_a:
                ab_copy(r, d).wait_send()
        return carry

    lax.fori_loop(0, nblk, drain, 0)
    if do_a:
        for g in range(len(rest)):
            for d in ORDER:
                rest_copy(g, d).wait_send()


def update_call(do_c, do_a, outgoing, cid, z, t, mask, vecs, mats):
    nrow, _, ncol = z.shape
    nblk = nrow // RB
    hbm = pl.BlockSpec(memory_space=pl.ANY)
    vmem = pl.BlockSpec(memory_space=pltpu.VMEM)
    sems = pltpu.SemaphoreType.DMA((nblk, NDEV))
    strided = pltpu.VMEM((ncol // LANES, CH * RB, LANES), jnp.float32)
    t_shape = jax.ShapeDtypeStruct((NDEV, SUB, nrow, ncol), jnp.bfloat16)
    args, in_specs, outs = [z], [hbm], []
    scratch = [pltpu.VMEM((RB, CH, ncol), jnp.bfloat16), strided, pltpu.VMEM((CH, ncol), jnp.bfloat16), pltpu.SemaphoreType.DMA]
    if do_c:
        args.append(t)
        in_specs.append(hbm)
        outs += [jax.ShapeDtypeStruct(z.shape, jnp.bfloat16), t_shape]
        scratch += [pltpu.VMEM((CH, ncol), jnp.float32), pltpu.VMEM((CH, ncol), jnp.float32), pltpu.VMEM((CH, ncol), jnp.bfloat16),
                    pltpu.VMEM((NDEV, SUB, RB, ncol), jnp.bfloat16), sems, sems, pltpu.SemaphoreType.DMA((NDEV,))]
    if do_a:
        args.append(mask)
        in_specs.append(vmem)
        nrest = len(first_and_rest(do_c)[1])
        rsems = pltpu.SemaphoreType.DMA((nrest, NDEV))
        outs += [t_shape, jax.ShapeDtypeStruct((NDEV, SUB, 2, nrow, ncol), jnp.bfloat16)]
        scratch += [pltpu.VMEM((4 * CH, ncol), jnp.float32), strided, pltpu.VMEM((NDEV, SUB, 2, RB, ncol), jnp.bfloat16),
                    pltpu.VMEM((NDEV, SUB, 2, nrow, ncol), jnp.bfloat16), pltpu.VMEM((2, NDEV, nrow, ncol), jnp.bfloat16),
                    sems, sems, pltpu.SemaphoreType.DMA((nblk,)), pltpu.SemaphoreType.DMA, pltpu.SemaphoreType.DMA((2,)), rsems, rsems, pltpu.SemaphoreType.DMA]
    args += [vecs, mats]
    in_specs += [vmem, vmem]
    return pl.pallas_call(
        functools.partial(update_kernel, do_c, do_a, outgoing, nrow, ncol),
        in_specs=in_specs,
        out_specs=[hbm] * len(outs),
        out_shape=outs,
        scratch_shapes=scratch,
        compiler_params=pltpu.CompilerParams(collective_id=cid, has_side_effects=True, vmem_limit_bytes=VMEM_LIMIT),
        name="update",
    )(*args)


def solution(mesh):
    row_spec = P(ALL_ROWS, None, None)
    mask_spec = P(ALL_ROWS, None)

    def local_stack(pair_rep, pair_mask, norm_in, norm_out, w_ab, w_gate, w_out):
        mask_f = pair_mask.astype(jnp.float32)[:, None, :]
        n_layers = w_ab.shape[0]
        n_upd = 2 * n_layers
        n_in = norm_in.astype(jnp.float32).reshape(n_upd, 2, CH)
        n_out = norm_out.astype(jnp.float32).reshape(n_upd, 2, CH)
        n_next = jnp.roll(n_in, -1, axis=0)
        vecs = jnp.stack([n_in[:, 0], n_in[:, 1], n_out[:, 0], n_out[:, 1], n_next[:, 0], n_next[:, 1]], axis=-1)

        def rows_of(w):
            return jnp.swapaxes(w.reshape(n_upd, *w.shape[2:]), 1, 2)

        mats = jnp.concatenate([rows_of(w_gate), rows_of(w_out), jnp.roll(rows_of(w_ab), -1, axis=0)], axis=1)

        def to_incoming(l, z, t):
            z, _, t, _ = update_call(True, True, False, 1, z, t, mask_f, vecs[2 * l], mats[2 * l])
            return z, t

        def body(l, state):
            z, t = to_incoming(l, *state)
            z, _, t, _ = update_call(True, True, True, 2, z, t, mask_f, vecs[2 * l + 1], mats[2 * l + 1])
            return z, t

        z = jnp.swapaxes(pair_rep, 1, 2)
        t, _ = update_call(False, True, True, 0, z, None, mask_f, vecs[n_upd - 1], mats[n_upd - 1])
        z, t = lax.fori_loop(0, n_layers - 1, body, (z, t))
        z, t = to_incoming(n_layers - 1, z, t)
        z, _ = update_call(True, False, False, 3, z, t, mask_f, vecs[n_upd - 1], mats[n_upd - 1])
        return jnp.swapaxes(z, 1, 2)

    return jax.shard_map(local_stack, mesh=mesh, in_specs=(row_spec, mask_spec, P(), P(), P(), P(), P()), out_specs=row_spec, check_vma=False)
```

```python
import functools

import jax
import jax.numpy as jnp
from jax import lax
from jax.experimental import pallas as pl
from jax.experimental.pallas import tpu as pltpu
from jax.sharding import PartitionSpec as P

LN_EPS = 1e-5
ALL_ROWS = ("data", "dap2", "dap")
MESH = pl.DeviceIdType.MESH
NDEV = 8
CH = 128
SUB = CH // NDEV
RB = 16
LANES = 128
VMEM_LIMIT = 62 * 1024 * 1024
ORDER = (6, 4, 2, 7, 5, 3, 1)


def norm_cols(vals, gain, shift):
    mean_val = jnp.mean(vals, axis=0, keepdims=True)
    centered = vals - mean_val
    var_val = jnp.mean(centered * centered, axis=0, keepdims=True)
    return centered * lax.rsqrt(var_val + LN_EPS) * gain + shift


def sigmoid(vals):
    return 0.5 * jnp.tanh(0.5 * vals) + 0.5


def first_and_rest(do_c):
    return (4, ((4, 4), (8, 4), (12, 3), (15, 1))) if do_c else (8, ((8, 4), (12, 3), (15, 1)))


def update_kernel(do_c, do_a, outgoing, nrow, ncol, *refs):
    refs = list(refs)

    def take(count):
        out = refs[:count]
        del refs[:count]
        return out

    z_ref, = take(1)
    if do_c:
        t_ref, = take(1)
    if do_a:
        m_hbm, = take(1)
    v_hbm, w_hbm = take(2)
    if do_c:
        zo_ref, tr_ref = take(2)
    if do_a:
        tn_ref, ab_ref = take(2)
    zbuf, scr, x_ref, l_z, v_ref, w_ref, l_par = take(7)
    if do_c:
        o_ref, g_ref, y_ref, tblk, s_t, r_t, l_t = take(7)
    if do_a:
        p_ref, scr_b, abblk, recv, tst, s_ab, r_ab, l_ab, l_st, l_tn, s_rest, r_rest, l_rest, m_ref = take(14)

    y_id = lax.axis_index("dap2")
    xc_id = lax.axis_index("dap")
    z_id = lax.axis_index("data")
    x_id, c_id = xc_id // 2, xc_id % 2
    me = y_id * 4 + xc_id
    nblk = nrow // RB
    first, rest = first_and_rest(do_c)

    def peer(d):
        py, px, pc = (y_id + d // 4) % 2, (x_id + (d // 2) % 2) % 2, (c_id + d % 2) % 2
        return (z_id, py, px * 2 + pc), py * 4 + px * 2 + pc

    def rows(r):
        return pl.ds(r * RB, RB)

    def t_copy(r, d):
        dev, num = peer(d)
        return pltpu.make_async_remote_copy(
            src_ref=t_ref.at[num, :, rows(r)], dst_ref=tr_ref.at[me, :, rows(r)],
            send_sem=s_t.at[r, d], recv_sem=r_t.at[r, d], device_id=dev, device_id_type=MESH)

    def ab_copy(r, d):
        dev, num = peer(d)
        return pltpu.make_async_remote_copy(
            src_ref=ab_ref.at[num, pl.ds(0, first), :, rows(r)], dst_ref=recv.at[me, pl.ds(0, first), :, rows(r)],
            send_sem=s_ab.at[r, d], recv_sem=r_ab.at[r, d], device_id=dev, device_id_type=MESH)

    def own_ab(r):
        return pltpu.make_async_copy(ab_ref.at[me, pl.ds(0, first), :, rows(r)], recv.at[me, pl.ds(0, first), :, rows(r)], l_ab.at[r])

    def rest_copy(g, d):
        dev, num = peer(d)
        return pltpu.make_async_remote_copy(
            src_ref=ab_ref.at[num, pl.ds(*rest[g])], dst_ref=recv.at[me, pl.ds(*rest[g])],
            send_sem=s_rest.at[g, d], recv_sem=r_rest.at[g, d], device_id=dev, device_id_type=MESH)

    def own_rest():
        return pltpu.make_async_copy(ab_ref.at[me, pl.ds(first, SUB - first)], recv.at[me, pl.ds(first, SUB - first)], l_rest)

    def stage_ab(r):
        return pltpu.make_async_copy(abblk, ab_ref.at[:, :, :, rows(r)], l_st)

    def load_t(r, d):
        num = peer(d)[1]
        src_ref = t_ref if d == 0 else tr_ref
        return pltpu.make_async_copy(src_ref.at[num, :, rows(r)], tblk.at[num], l_t.at[d])

    def load_z(r):
        return pltpu.make_async_copy(z_ref.at[rows(r)], zbuf, l_z)

    def store_z(r):
        return pltpu.make_async_copy(zbuf, zo_ref.at[rows(r)], l_z)

    barrier = pltpu.get_barrier_semaphore()
    for d in range(1, NDEV):
        pl.semaphore_signal(barrier, inc=1, device_id=peer(d)[0], device_id_type=MESH)
    pl.semaphore_wait(barrier, NDEV - 1)

    if do_c:
        for r in range(nblk):
            for d in ORDER:
                t_copy(r, d).start()

    params = [(v_hbm, v_ref), (w_hbm, w_ref)] + ([(m_hbm, m_ref)] if do_a else [])
    loads = [pltpu.make_async_copy(src, dst, l_par.at[n]) for n, (src, dst) in enumerate(params)]
    for load in loads:
        load.start()
    for load in loads:
        load.wait()

    chunks = [pl.ds(l0, LANES) for l0 in range(0, ncol, LANES)]

    def one_row(r, i):
        if do_c:
            for q, ln in enumerate(chunks):
                x_ref[:, ln] = norm_cols(zbuf[i, :, ln].astype(jnp.float32), v_ref[:, 0:1], v_ref[:, 1:2]).astype(jnp.bfloat16)
                y_ref[:, ln] = norm_cols(scr[q, pl.ds(i, CH, stride=RB), :], v_ref[:, 2:3], v_ref[:, 3:4]).astype(jnp.bfloat16)
            g_ref[...] = jnp.dot(w_ref[pl.ds(0, CH), :], x_ref[...], preferred_element_type=jnp.float32)
            o_ref[...] = jnp.dot(w_ref[pl.ds(CH, CH), :], y_ref[...], preferred_element_type=jnp.float32)
            for q, ln in enumerate(chunks):
                new_z = zbuf[i, :, ln].astype(jnp.float32) + sigmoid(g_ref[:, ln]) * o_ref[:, ln]
                zbuf[i, :, ln] = new_z.astype(jnp.bfloat16)
        if do_a:
            for q, ln in enumerate(chunks):
                x_ref[:, ln] = norm_cols(zbuf[i, :, ln].astype(jnp.float32), v_ref[:, 4:5], v_ref[:, 5:6]).astype(jnp.bfloat16)
            p_ref[...] = jnp.dot(w_ref[pl.ds(2 * CH, 4 * CH), :], x_ref[...], preferred_element_type=jnp.float32)
            for q, ln in enumerate(chunks):
                keep = m_ref[r * RB + i, :, ln]
                scr[q, pl.ds(i, CH, stride=RB), :] = keep * sigmoid(p_ref[pl.ds(CH, CH), ln]) * p_ref[pl.ds(0, CH), ln]
                scr_b[q, pl.ds(i, CH, stride=RB), :] = keep * sigmoid(p_ref[pl.ds(3 * CH, CH), ln]) * p_ref[pl.ds(2 * CH, CH), ln]

    def block_step(r, carry):
        load_z(r).start()
        if do_c:
            for d in ORDER:
                t_copy(r, d).wait_recv()
            for d in range(NDEV):
                load_t(r, d).start()
            for d in range(NDEV):
                load_t(r, d).wait()
            for s in range(NDEV):
                for q, ln in enumerate(chunks):
                    scr[q, pl.ds(s * SUB * RB, SUB * RB), :] = tblk[s, :, :, ln].astype(jnp.float32).reshape(SUB * RB, LANES)
        load_z(r).wait()

        def row_step(i, inner):
            one_row(r, i)
            return inner

        lax.fori_loop(0, RB, row_step, 0)
        if do_c:
            store_z(r).start()
        if do_a:
            for d in range(NDEV):
                for s_ref, u in ((scr, 0), (scr_b, 1)):
                    for q, ln in enumerate(chunks):
                        abblk[d, :, u, :, ln] = s_ref[q, pl.ds(d * SUB * RB, SUB * RB), :].reshape(SUB, RB, LANES).astype(jnp.bfloat16)
            stage_ab(r).start()
            stage_ab(r).wait()
            for d in ORDER:
                ab_copy(r, d).start()
            own_ab(r).start()
        if do_c:
            store_z(r).wait()
        return carry

    lax.fori_loop(0, nblk, block_step, 0)

    if do_a:
        for g in range(len(rest)):
            for d in ORDER:
                rest_copy(g, d).start()
        own_rest().start()

        def wait_ab(r, carry):
            for d in ORDER:
                ab_copy(r, d).wait_recv()
            own_ab(r).wait()
            return carry

        lax.fori_loop(0, nblk, wait_ab, 0)
        own_rest().wait()

        def put_t(ch):
            return pltpu.make_async_copy(tst.at[ch % 2], tn_ref.at[:, ch], l_tn.at[ch % 2])

        def chan_step(ch, carry):
            for g in range(len(rest)):
                @pl.when(ch == rest[g][0])
                def _(g=g):
                    for d in ORDER:
                        rest_copy(g, d).wait_recv()

            a_val = recv[:, ch, 0].reshape(NDEV * nrow, ncol)
            b_val = recv[:, ch, 1].reshape(NDEV * nrow, ncol)
            dims = (((1,), (1,)), ((), ())) if outgoing else (((0,), (0,)), ((), ()))
            t_val = lax.dot_general(a_val, b_val, dims, preferred_element_type=jnp.float32)

            @pl.when(ch >= 2)
            def _():
                put_t(ch - 2).wait()

            tst[ch % 2] = t_val.astype(jnp.bfloat16).reshape(NDEV, nrow, ncol)
            put_t(ch).start()
            return carry

        lax.fori_loop(0, SUB, chan_step, 0)
        put_t(SUB - 2).wait()
        put_t(SUB - 1).wait()

    def drain(r, carry):
        for d in ORDER:
            if do_c:
                t_copy(r, d).wait_send()
            if do_a:
                ab_copy(r, d).wait_send()
        return carry

    lax.fori_loop(0, nblk, drain, 0)
    if do_a:
        for g in range(len(rest)):
            for d in ORDER:
                rest_copy(g, d).wait_send()


def update_call(do_c, do_a, outgoing, cid, z, t, mask, vecs, mats):
    nrow, _, ncol = z.shape
    nblk = nrow // RB
    hbm = pl.BlockSpec(memory_space=pl.ANY)
    sems = pltpu.SemaphoreType.DMA((nblk, NDEV))
    strided = pltpu.VMEM((ncol // LANES, CH * RB, LANES), jnp.float32)
    t_shape = jax.ShapeDtypeStruct((NDEV, SUB, nrow, ncol), jnp.bfloat16)
    args, in_specs, outs = [z], [hbm], []
    scratch = [pltpu.VMEM((RB, CH, ncol), jnp.bfloat16), strided, pltpu.VMEM((CH, ncol), jnp.bfloat16), pltpu.SemaphoreType.DMA,
               pltpu.VMEM(vecs.shape, vecs.dtype), pltpu.VMEM(mats.shape, mats.dtype), pltpu.SemaphoreType.DMA((3,))]
    if do_c:
        args.append(t)
        in_specs.append(hbm)
        outs += [jax.ShapeDtypeStruct(z.shape, jnp.bfloat16), t_shape]
        scratch += [pltpu.VMEM((CH, ncol), jnp.float32), pltpu.VMEM((CH, ncol), jnp.float32), pltpu.VMEM((CH, ncol), jnp.bfloat16),
                    pltpu.VMEM((NDEV, SUB, RB, ncol), jnp.bfloat16), sems, sems, pltpu.SemaphoreType.DMA((NDEV,))]
    if do_a:
        args.append(mask)
        in_specs.append(hbm)
        nrest = len(first_and_rest(do_c)[1])
        rsems = pltpu.SemaphoreType.DMA((nrest, NDEV))
        outs += [t_shape, jax.ShapeDtypeStruct((NDEV, SUB, 2, nrow, ncol), jnp.bfloat16)]
        scratch += [pltpu.VMEM((4 * CH, ncol), jnp.float32), strided, pltpu.VMEM((NDEV, SUB, 2, RB, ncol), jnp.bfloat16),
                    pltpu.VMEM((NDEV, SUB, 2, nrow, ncol), jnp.bfloat16), pltpu.VMEM((2, NDEV, nrow, ncol), jnp.bfloat16),
                    sems, sems, pltpu.SemaphoreType.DMA((nblk,)), pltpu.SemaphoreType.DMA, pltpu.SemaphoreType.DMA((2,)), rsems, rsems, pltpu.SemaphoreType.DMA, pltpu.VMEM(mask.shape, mask.dtype)]
    args += [vecs, mats]
    in_specs += [hbm, hbm]
    return pl.pallas_call(
        functools.partial(update_kernel, do_c, do_a, outgoing, nrow, ncol),
        in_specs=in_specs,
        out_specs=[hbm] * len(outs),
        out_shape=outs,
        scratch_shapes=scratch,
        compiler_params=pltpu.CompilerParams(collective_id=cid, has_side_effects=True, vmem_limit_bytes=VMEM_LIMIT),
        name="update",
    )(*args)


def solution(mesh):
    row_spec = P(ALL_ROWS, None, None)
    mask_spec = P(ALL_ROWS, None)

    def local_stack(pair_rep, pair_mask, norm_in, norm_out, w_ab, w_gate, w_out):
        mask_f = pair_mask.astype(jnp.float32)[:, None, :]
        n_layers = w_ab.shape[0]
        n_upd = 2 * n_layers
        n_in = norm_in.astype(jnp.float32).reshape(n_upd, 2, CH)
        n_out = norm_out.astype(jnp.float32).reshape(n_upd, 2, CH)
        n_next = jnp.roll(n_in, -1, axis=0)
        vecs = jnp.stack([n_in[:, 0], n_in[:, 1], n_out[:, 0], n_out[:, 1], n_next[:, 0], n_next[:, 1]], axis=-1)

        def rows_of(w):
            return jnp.swapaxes(w.reshape(n_upd, *w.shape[2:]), 1, 2)

        mats = jnp.concatenate([rows_of(w_gate), rows_of(w_out), jnp.roll(rows_of(w_ab), -1, axis=0)], axis=1)

        def to_incoming(l, z, t):
            z, _, t, _ = update_call(True, True, False, 1, z, t, mask_f, vecs[2 * l], mats[2 * l])
            return z, t

        def body(l, state):
            z, t = to_incoming(l, *state)
            z, _, t, _ = update_call(True, True, True, 2, z, t, mask_f, vecs[2 * l + 1], mats[2 * l + 1])
            return z, t

        z = jnp.swapaxes(pair_rep, 1, 2)
        t, _ = update_call(False, True, True, 0, z, None, mask_f, vecs[n_upd - 1], mats[n_upd - 1])
        z, t = lax.fori_loop(0, n_layers - 1, body, (z, t))
        z, t = to_incoming(n_layers - 1, z, t)
        z, _ = update_call(True, False, False, 3, z, t, mask_f, vecs[n_upd - 1], mats[n_upd - 1])
        return jnp.swapaxes(z, 1, 2)

    return jax.shard_map(local_stack, mesh=mesh, in_specs=(row_spec, mask_spec, P(), P(), P(), P(), P()), out_specs=row_spec, check_vma=False)
```
